16 devices in a mesh: rep: 2 (over y, z), dp: 8 (over x, core).
Axes of the slice: x: 4, y: 2, z: 1, core: 2. Of those that a mesh axis runs over, the one named last changes fastest.
The devices are a block of a 4x4x8 slice.
Arguments:
- hidden: bfloat16 [512, 2048], P(('rep', 'dp')), parts along dimension 0
- lengths: int32 [512], P(('rep', 'dp')), parts along dimension 0
- kv_cache: bfloat16 [2, 512, 128, 576], P(None, ('rep', 'dp')), parts along dimension 1
- norm_attn: float32 [2, 2048], replicated
- w_q: bfloat16 [2, 2048, 9216], replicated
- w_o: bfloat16 [2, 8192, 2048], replicated
- norm_ffn: float32 [2, 2048], replicated
- w_gate: bfloat16 [2, 2048, 11264], P(None, None, 'dp')
- w_up: bfloat16 [2, 2048, 11264], P(None, None, 'dp')
- w_down: bfloat16 [2, 11264, 2048], P(None, 'dp')
- norm_final: float32 [2048], replicated
- w_head: bfloat16 [2048, 163840], P(None, 'dp')
Outputs:
- output: float32 [512, 163840], P('rep', 'dp'), parts along dimension 0
There are 2 independent parts. The reference program is written for one: setup_inputs(seed, part) draws one part's arguments, and reference() takes and returns one part's arrays. A program takes and returns all parts, laid end to end along the dimension named above; an argument that names none is the same for every part.
All inputs are finite; a program needn't handle non-finite values.
Results may differ from the reference program's by a relative error of at most 0.02.
Values are sent between devices in bfloat16 or wider.
A program may use at most 768 MiB of HBM per device.

```python
import jax
import jax.numpy as jnp
from jax import lax

BATCH_SIZE = 256
SEQ_LEN = 128
D_MODEL = 2048
NUM_HEADS = 16
FFN_DIM = 11264
VOCAB_SIZE = 163840
NUM_LAYERS = 2
LATENT_DIM = 512
ROPE_DIM = 64
KV_WIDTH = LATENT_DIM + ROPE_DIM
QK_SCALE = 192 ** -0.5
NORM_EPS = 1e-6


def setup_inputs(seed: int = 0, part: int = 0) -> dict:
    own_keys = jax.random.split(jax.random.fold_in(jax.random.key(seed), part), 3)
    shared_keys = jax.random.split(jax.random.key(seed + 1), 9)
    hidden = jax.random.normal(own_keys[0], (BATCH_SIZE, D_MODEL), jnp.float32)
    lengths = jax.random.randint(own_keys[1], (BATCH_SIZE,), 1, SEQ_LEN + 1, jnp.int32)
    lengths = lengths.at[0].set(SEQ_LEN)
    kv_cache = jax.random.normal(own_keys[2], (NUM_LAYERS, BATCH_SIZE, SEQ_LEN, KV_WIDTH), jnp.float32)
    attn_gain = SEQ_LEN ** 0.5 / 8.0
    norm_attn = jax.random.uniform(shared_keys[0], (NUM_LAYERS, D_MODEL), jnp.float32, 0.5, 1.5)
    w_q = jax.random.normal(shared_keys[1], (NUM_LAYERS, D_MODEL, NUM_HEADS * KV_WIDTH), jnp.float32) * D_MODEL ** -0.5
    w_o = jax.random.normal(shared_keys[2], (NUM_LAYERS, NUM_HEADS * LATENT_DIM, D_MODEL), jnp.float32) * ((NUM_HEADS * LATENT_DIM) ** -0.5 * attn_gain)
    norm_ffn = jax.random.uniform(shared_keys[3], (NUM_LAYERS, D_MODEL), jnp.float32, 0.5, 1.5)
    w_gate = jax.random.normal(shared_keys[4], (NUM_LAYERS, D_MODEL, FFN_DIM), jnp.float32) * D_MODEL ** -0.5
    w_up = jax.random.normal(shared_keys[5], (NUM_LAYERS, D_MODEL, FFN_DIM), jnp.float32) * D_MODEL ** -0.5
    w_down = jax.random.normal(shared_keys[6], (NUM_LAYERS, FFN_DIM, D_MODEL), jnp.float32) * (2.0 * FFN_DIM ** -0.5)
    norm_final = jax.random.uniform(shared_keys[7], (D_MODEL,), jnp.float32, 0.5, 1.5)
    w_head = jax.random.normal(shared_keys[8], (D_MODEL, VOCAB_SIZE), jnp.float32) * D_MODEL ** -0.5
    return dict(
        hidden=hidden.astype(jnp.bfloat16),
        lengths=lengths,
        kv_cache=kv_cache.astype(jnp.bfloat16),
        norm_attn=norm_attn,
        w_q=w_q.astype(jnp.bfloat16),
        w_o=w_o.astype(jnp.bfloat16),
        norm_ffn=norm_ffn,
        w_gate=w_gate.astype(jnp.bfloat16),
        w_up=w_up.astype(jnp.bfloat16),
        w_down=w_down.astype(jnp.bfloat16),
        norm_final=norm_final,
        w_head=w_head.astype(jnp.bfloat16),
    )


def rms_norm(x_rows, gain_vec):
    x_float = x_rows.astype(jnp.float32)
    inv_rms = lax.rsqrt(jnp.mean(x_float * x_float, axis=-1, keepdims=True) + NORM_EPS)
    return (x_float * inv_rms * gain_vec).astype(jnp.bfloat16)


def attend_row(row_args):
    q_heads, cache_row, length = row_args
    cache_float = cache_row.astype(jnp.float32)
    scores = jnp.dot(q_heads.astype(jnp.float32), cache_float.T, preferred_element_type=jnp.float32) * QK_SCALE
    key_valid = jnp.arange(cache_row.shape[0]) < length
    scores = jnp.where(key_valid[None, :], scores, -1e30)
    attn_probs = jax.nn.softmax(scores, axis=-1).astype(jnp.bfloat16)
    context = jnp.dot(attn_probs.astype(jnp.float32), cache_float[:, :LATENT_DIM], preferred_element_type=jnp.float32)
    return context.astype(jnp.bfloat16)


def reference(hidden, lengths, kv_cache, norm_attn, w_q, w_o, norm_ffn, w_gate, w_up, w_down, norm_final, w_head):
    num_rows = hidden.shape[0]

    def layer_step(x_rows, layer_args):
        layer_cache, attn_norm, wq_layer, wo_layer, ffn_norm, gate_layer, up_layer, down_layer = layer_args
        normed = rms_norm(x_rows, attn_norm)
        q_all = jnp.dot(normed, wq_layer, preferred_element_type=jnp.float32).astype(jnp.bfloat16)
        q_all = q_all.reshape(num_rows, NUM_HEADS, KV_WIDTH)
        context = lax.map(attend_row, (q_all, layer_cache, lengths)).reshape(num_rows, NUM_HEADS * LATENT_DIM)
        x_rows = (x_rows.astype(jnp.float32) + jnp.dot(context, wo_layer, preferred_element_type=jnp.float32)).astype(jnp.bfloat16)
        normed = rms_norm(x_rows, ffn_norm)
        gate_proj = jnp.dot(normed, gate_layer, preferred_element_type=jnp.float32)
        up_proj = jnp.dot(normed, up_layer, preferred_element_type=jnp.float32)
        act_rows = (jax.nn.silu(gate_proj) * up_proj).astype(jnp.bfloat16)
        ffn_out = jnp.dot(act_rows, down_layer, preferred_element_type=jnp.float32)
        x_rows = (x_rows.astype(jnp.float32) + ffn_out).astype(jnp.bfloat16)
        return x_rows, None

    layer_inputs = (kv_cache, norm_attn, w_q, w_o, norm_ffn, w_gate, w_up, w_down)
    x_final, layer_outs = lax.scan(layer_step, hidden, layer_inputs)
    normed = rms_norm(x_final, norm_final)
    return jnp.dot(normed, w_head, preferred_element_type=jnp.float32)
```

```python
import functools

import jax
import jax.numpy as jnp
from jax import lax
from jax.experimental import pallas as pl
from jax.experimental.pallas import tpu as pltpu
from jax.sharding import PartitionSpec as P

LATENT_DIM = 512
QK_SCALE = 192 ** -0.5
NORM_EPS = 1e-6
MESH = pl.DeviceIdType.MESH
BF16, F32 = jnp.bfloat16, jnp.float32
TILE = 256
LANES = 128
GROUP = 8


def rms_norm(x_float, gain_row):
    inv_rms = lax.rsqrt(jnp.mean(x_float * x_float, axis=-1, keepdims=True) + NORM_EPS)
    return (x_float * inv_rms * gain_row).astype(BF16)


def decode_kernel(cfg, lengths, hidden, kv_hbm, norm_attn, wq_hbm, wo_hbm, norm_ffn, wg_hbm, wu_hbm, wd_hbm, norm_final,
                  out, wa, wb, kv_b, x_full, h_s, q_s, o_s, o_all, xg, act, y_send, y_recv, y_sum, relay_in, relay_out,
                  direct_in, w_sem, kv_sem, x_send, x_recv, q_send, q_recv, o_send, o_recv, ag_send, ag_recv,
                  d2d_send, d2d_recv, y_ssem, y_rsem, rs_send, rs_recv):
    num_layers, rows, heads, width, d_model, ffn, n_dev = cfg
    chips = n_dev // 2
    pair = 2 * rows
    half_d = d_model // 2
    half_h = heads // 2
    q_cols = half_h * width
    t_tiles = half_d // TILE
    q_parts = q_s.shape[0]

    me = lax.axis_index("dp")
    chip, core = lax.div(me, 2), lax.rem(me, 2)
    other = 1 - core
    partner = chip * 2 + other
    right_chip, left_chip = lax.rem(chip + 1, chips), lax.rem(chip + chips - 1, chips)
    far_chip = lax.rem(chip + 2, chips)
    right, left = right_chip * 2 + core, left_chip * 2 + core

    def remote(src, dst, send_sem, recv_sem, device):
        return pltpu.make_async_remote_copy(src_ref=src, dst_ref=dst, send_sem=send_sem, recv_sem=recv_sem,
                                            device_id={"dp": device}, device_id_type=MESH)

    pair_cols = 2 * width
    n_q = q_cols // pair_cols
    n_o = 4
    o_depth = wo_hbm.shape[1] // n_o
    kv_parts = rows // GROUP

    def q_copy(l, p):
        col = pl.multiple_of(core * q_cols + p * pair_cols, LANES)
        return pltpu.make_async_copy(wq_hbm.at[l, :, pl.ds(col, pair_cols)],
                                     wa.at[:, p * pair_cols:(p + 1) * pair_cols], w_sem.at[p])

    def o_copy(l, p):
        col = pl.multiple_of(core * half_d, LANES)
        return pltpu.make_async_copy(wo_hbm.at[l, p * o_depth:(p + 1) * o_depth, pl.ds(col, half_d)],
                                     wb.at[p * o_depth:(p + 1) * o_depth, :], w_sem.at[n_q + p])

    def ffn_copies(l):
        return [pltpu.make_async_copy(wg_hbm.at[l], wa.at[:, 0:ffn], w_sem.at[n_q + n_o]),
                pltpu.make_async_copy(wu_hbm.at[l], wa.at[:, ffn:2 * ffn], w_sem.at[n_q + n_o + 1]),
                pltpu.make_async_copy(wd_hbm.at[l], wa.at[0:ffn, 2 * ffn:2 * ffn + d_model], w_sem.at[n_q + n_o + 2])]

    def kv_copy(l, g):
        return pltpu.make_async_copy(kv_hbm.at[l, g * GROUP:(g + 1) * GROUP],
                                     kv_b.at[g * GROUP:(g + 1) * GROUP], kv_sem.at[g])

    for p in range(n_q):
        q_copy(0, p).start()
    for g in range(kv_parts):
        kv_copy(0, g).start()
    for p in range(n_o):
        o_copy(0, p).start()

    barrier = pltpu.get_barrier_semaphore()
    for device in (partner, left, right):
        pl.semaphore_signal(barrier, inc=1, device_id={"dp": device}, device_id_type=MESH)
    pl.semaphore_wait(barrier, 3)

    if width % LANES:
        q_s[q_parts - 1] = jnp.zeros(q_s.shape[1:], F32)

    own_rows = pl.ds(pl.multiple_of(core * rows, rows), rows)
    first = remote(hidden, x_full.at[own_rows, :], x_send.at[0], x_recv.at[0], partner)
    first.start()
    x_full[own_rows, :] = hidden[...]
    first.wait()

    def half_cols(which, t=0, n=None):
        return pl.ds(pl.multiple_of(which * half_d + t * TILE, LANES), half_d if n is None else n)

    def gather_rows(gain_row, dst):
        def piece(which_chip, half, count=rows):
            return xg.at[pl.ds(pl.multiple_of(which_chip * pair + half * rows, rows), count), half_cols(core)]

        def send(which_chip, half, slot, device):
            copy = remote(piece(which_chip, half), piece(which_chip, half), ag_send.at[slot], ag_recv.at[slot], device)
            copy.start()
            return copy

        def pass_on(which_chip, half, slot, count=rows):
            copy = remote(piece(which_chip, half, count), piece(which_chip, half, count),
                          d2d_send.at[slot], d2d_recv.at[slot], partner)
            copy.start()
            return copy

        def norm(which_chip):
            at = pl.ds(pl.multiple_of(which_chip * pair, pair), pair)
            dst[at, :] = rms_norm(xg[at, :].astype(F32), gain_row)

        own_a = send(chip, 0, 0, right)
        own_b = send(chip, 1, 1, left)
        own_b2 = send(chip, 1, 2, right)
        own_a2 = send(chip, 0, 3, left)
        passed = [pass_on(chip, 0, 0, pair)]
        own_a.wait_recv()
        far_a = send(left_chip, 0, 4, right)
        own_b.wait_recv()
        far_b = send(right_chip, 1, 5, left)
        passed.append(pass_on(left_chip, 0, 1))
        passed.append(pass_on(right_chip, 1, 2))
        passed[0].wait_recv()
        norm(chip)
        own_b2.wait_recv()
        passed.append(pass_on(left_chip, 1, 3))
        own_a2.wait_recv()
        passed.append(pass_on(right_chip, 0, 4))
        passed[1].wait_recv()
        passed[3].wait_recv()
        norm(left_chip)
        passed[2].wait_recv()
        passed[4].wait_recv()
        norm(right_chip)
        far_a.wait_recv()
        passed.append(pass_on(far_chip, 0, 5))
        far_b.wait_recv()
        passed.append(pass_on(far_chip, 1, 6))
        passed[5].wait_recv()
        passed[6].wait_recv()
        norm(far_chip)
        for copy in [own_a, own_b, own_b2, own_a2, far_a, far_b] + passed:
            copy.wait_send()

    own_chip_rows = pl.ds(pl.multiple_of(chip * pair, pair), pair)

    for layer in range(num_layers):
        h_s[...] = rms_norm(x_full[...].astype(F32), norm_attn[layer:layer + 1, :])
        q_copies = []
        for p in range(n_q):
            q_copy(layer, p).wait()
            q_val = jnp.dot(h_s[...], wa[:, p * pair_cols:(p + 1) * pair_cols], preferred_element_type=F32)
            q_val = q_val.astype(BF16).astype(F32)
            for e in range(2):
                head = core * half_h + 2 * p + e
                base = pl.multiple_of(head * pair, pair)
                q_head = q_val[:, e * width:(e + 1) * width]
                for c in range(q_parts):
                    lanes = min(LANES, width - c * LANES)
                    q_s[c, pl.ds(base, pair), 0:lanes] = q_head[:, c * LANES:c * LANES + lanes]
                away = pl.ds(pl.multiple_of(base + other * rows, rows), rows)
                copy = remote(q_s.at[:, away, :], q_s.at[:, away, :], q_send.at[2 * p + e], q_recv.at[2 * p + e], partner)
                copy.start()
                q_copies.append(copy)
        for copy in ffn_copies(layer):
            copy.start()
        for copy in q_copies:
            copy.wait_recv()

        o_copies = []
        per_half = kv_parts // 2
        key_pos = lax.broadcasted_iota(jnp.int32, (heads, kv_b.shape[1]), 1)
        for half in range(2):
            for g in range(half * per_half, (half + 1) * per_half):
                kv_copy(layer, g).wait()
                scores = []
                for i in range(GROUP):
                    b = g * GROUP + i
                    at = pl.ds(core * rows + b, heads, stride=pair)
                    q_b = jnp.concatenate([q_s[c, at, :] for c in range(q_parts)], axis=1)[:, 0:width].astype(BF16)
                    s_b = lax.dot_general(q_b, kv_b[b], (((1,), (1,)), ((), ())), preferred_element_type=F32) * QK_SCALE
                    scores.append(jnp.where(key_pos < lengths[b], s_b, -1e30))
                s_all = jnp.concatenate(scores, axis=0)
                e_all = jnp.exp(s_all - jnp.max(s_all, axis=-1, keepdims=True))
                p_all = (e_all / jnp.sum(e_all, axis=-1, keepdims=True)).astype(BF16)
                for i in range(GROUP):
                    b = g * GROUP + i
                    o_b = jnp.dot(p_all[i * heads:(i + 1) * heads, :], kv_b[b, :, 0:LATENT_DIM], preferred_element_type=F32)
                    for c in range(LATENT_DIM // LANES):
                        o_s[c, pl.ds(b, heads, stride=rows), :] = o_b[:, c * LANES:(c + 1) * LANES]
                if layer + 1 < num_layers:
                    kv_copy(layer + 1, g).start()
            part = rows // 2
            at = pl.ds(pl.multiple_of(core * rows + half * part, part), part)
            for head in range(heads):
                for c in range(LATENT_DIM // LANES):
                    o_all[at, head * LATENT_DIM + c * LANES:head * LATENT_DIM + (c + 1) * LANES] = \
                        o_s[c, head * rows + half * part:head * rows + (half + 1) * part, :].astype(BF16)
            copy = remote(o_all.at[at, :], o_all.at[at, :], o_send.at[half], o_recv.at[half], partner)
            copy.start()
            o_copies.append(copy)
        for copy in q_copies:
            copy.wait_send()

        for p in range(n_o):
            o_copy(layer, p).wait()
        for copy in o_copies:
            copy.wait_recv()

        def wo_tile(t, carry):
            cols = pl.ds(pl.multiple_of(t * TILE, TILE), TILE)
            o_val = jnp.dot(o_all[...], wb[:, cols], preferred_element_type=F32)
            xg[own_chip_rows, half_cols(core, t, TILE)] = \
                (x_full[:, half_cols(core, t, TILE)].astype(F32) + o_val).astype(BF16)
            return carry

        lax.fori_loop(0, t_tiles, wo_tile, 0)
        for copy in o_copies:
            copy.wait_send()
        if layer + 1 < num_layers:
            for p in range(n_o):
                o_copy(layer + 1, p).start()

        gather_rows(norm_ffn[layer:layer + 1, :], out)
        for copy in ffn_copies(layer):
            copy.wait()

        def gate_up(j, carry):
            at = pl.ds(pl.multiple_of(j * LANES, LANES), LANES)
            at_up = pl.ds(pl.multiple_of(ffn + j * LANES, LANES), LANES)
            both = jnp.concatenate([wa[:, at], wa[:, at_up]], axis=1)
            val = jnp.dot(out[...], both, preferred_element_type=F32)
            act[:, at] = (jax.nn.silu(val[:, :LANES]) * val[:, LANES:]).astype(BF16)
            return carry

        lax.fori_loop(0, ffn // LANES, gate_up, 0)

        def down(which, t):
            cols = pl.ds(pl.multiple_of(2 * ffn + which * half_d + t * TILE, LANES), TILE)
            return jnp.dot(act[...], wa[0:ffn, cols], preferred_element_type=F32)

        y_copies = []
        for t in range(t_tiles):
            y_send[t] = down(other, t)
            copy = remote(y_send.at[t], y_recv.at[t], y_ssem.at[t], y_rsem.at[t], partner)
            copy.start()
            y_copies.append(copy)

        def rows_of(which_chip, half):
            return pl.ds(pl.multiple_of(which_chip * pair + half * rows, rows), rows)

        def rs_copy(src, dst, slot, t, device):
            copy = remote(src, dst, rs_send.at[slot, t], rs_recv.at[slot, t], device)
            copy.start()
            return copy

        rs_relay, rs_direct, rs_final = [], [], []

        def relay(t):
            for d, device, target in ((0, right, right_chip), (1, left, left_chip)):
                rs_relay[t][d].wait_recv()
                relay_out[d, t] = relay_in[d, t] + y_sum[t, rows_of(target, d), :]
                rs_final[t].append(rs_copy(relay_out.at[d, t], direct_in.at[2 + d, t], 4 + d, t, device))

        for t in range(t_tiles):
            own = down(core, t)
            y_copies[t].wait_recv()
            y_sum[t] = own + y_recv[t]
            rs_relay.append([rs_copy(y_sum.at[t, rows_of(far_chip, 0), :], relay_in.at[0, t], 0, t, right),
                             rs_copy(y_sum.at[t, rows_of(far_chip, 1), :], relay_in.at[1, t], 1, t, left)])
            rs_direct.append([rs_copy(y_sum.at[t, rows_of(right_chip, 1), :], direct_in.at[0, t], 2, t, right),
                              rs_copy(y_sum.at[t, rows_of(left_chip, 0), :], direct_in.at[1, t], 3, t, left)])
            rs_final.append([])
            if t >= 1:
                relay(t - 1)
        relay(t_tiles - 1)
        if layer + 1 < num_layers:
            for p in range(n_q):
                q_copy(layer + 1, p).start()

        last = layer + 1 == num_layers
        x_copies = []
        for t in range(t_tiles):
            for copy in rs_direct[t] + rs_final[t]:
                copy.wait_recv()
            cols = half_cols(core, t, TILE)
            for half in range(2):
                total = (y_sum[t, rows_of(chip, half), :] + direct_in[2 + half, t]) + direct_in[1 - half, t]
                x_new = (xg[rows_of(chip, half), cols].astype(F32) + total).astype(BF16)
                if last:
                    xg[rows_of(chip, half), cols] = x_new
                else:
                    x_full[half * rows:(half + 1) * rows, cols] = x_new
            if not last:
                copy = remote(x_full.at[:, cols], x_full.at[:, cols], x_send.at[1 + t], x_recv.at[1 + t], partner)
                copy.start()
                x_copies.append(copy)
        for copy in y_copies:
            copy.wait_send()
        for group in rs_relay + rs_direct + rs_final:
            for copy in group:
                copy.wait_send()
        for copy in x_copies:
            copy.wait()

    gather_rows(norm_final[0:1, :], out)


def decode_layers(n_dev, lengths, hidden, kv_cache, norm_attn, w_q, w_o, norm_ffn, w_gate, w_up, w_down, norm_final):
    num_layers, rows, seq_len, width = kv_cache.shape
    d_model = hidden.shape[1]
    heads = w_q.shape[2] // width
    ffn = w_gate.shape[2]
    pair, group_rows, half_d = 2 * rows, n_dev * rows, d_model // 2
    q_cols = heads * width // 2
    wa_cols = max(q_cols, 2 * ffn + d_model)
    wa_cols = -(-wa_cols // LANES) * LANES
    t_tiles = half_d // TILE
    pad_width = -(-width // LANES) * LANES
    hbm, vmem = pl.BlockSpec(memory_space=pl.ANY), pl.BlockSpec(memory_space=pltpu.VMEM)
    smem = pl.BlockSpec(memory_space=pltpu.SMEM)
    dma = pltpu.SemaphoreType.DMA
    cfg = (num_layers, rows, heads, width, d_model, ffn, n_dev)
    n_q = q_cols // (2 * width)
    scratch = [
        pltpu.VMEM((d_model, wa_cols), BF16),
        pltpu.VMEM((w_o.shape[1], half_d), BF16),
        pltpu.VMEM((rows, seq_len, width), BF16),
        pltpu.VMEM((pair, d_model), BF16),
        pltpu.VMEM((pair, d_model), BF16),
        pltpu.VMEM((pad_width // LANES, heads * pair, LANES), F32),
        pltpu.VMEM((LATENT_DIM // LANES, heads * rows, LANES), F32),
        pltpu.VMEM((pair, heads * LATENT_DIM), BF16),
        pltpu.VMEM((group_rows, d_model), BF16),
        pltpu.VMEM((group_rows, ffn), BF16),
        pltpu.VMEM((t_tiles, group_rows, TILE), F32),
        pltpu.VMEM((t_tiles, group_rows, TILE), F32),
        pltpu.VMEM((t_tiles, group_rows, TILE), F32),
        pltpu.VMEM((2, t_tiles, rows, TILE), F32),
        pltpu.VMEM((2, t_tiles, rows, TILE), F32),
        pltpu.VMEM((4, t_tiles, rows, TILE), F32),
        dma((n_q + 4 + 3,)),
        dma((rows // GROUP,)),
        dma((1 + t_tiles,)), dma((1 + t_tiles,)),
        dma((2 * n_q,)), dma((2 * n_q,)),
        dma((2,)), dma((2,)),
        dma((6,)), dma((6,)),
        dma((7,)), dma((7,)),
        dma((t_tiles,)), dma((t_tiles,)),
        dma((6, t_tiles)), dma((6, t_tiles)),
    ]
    return pl.pallas_call(
        functools.partial(decode_kernel, cfg),
        out_shape=jax.ShapeDtypeStruct((group_rows, d_model), BF16),
        in_specs=[smem, vmem, hbm, vmem, hbm, hbm, vmem, hbm, hbm, hbm, vmem],
        out_specs=vmem,
        scratch_shapes=scratch,
        compiler_params=pltpu.CompilerParams(collective_id=0, has_side_effects=True, vmem_limit_bytes=64 * 1000 * 1000),
        name="decode_layers",
    )(lengths, hidden, kv_cache, norm_attn, w_q, w_o, norm_ffn, w_gate, w_up, w_down, norm_final.reshape(1, -1))


def solution(mesh):
    row_axes = ('rep', 'dp')
    specs_in = (P(row_axes, None), P(row_axes), P(None, row_axes, None, None), P(), P(), P(), P(),
                P(None, None, 'dp'), P(None, None, 'dp'), P(None, 'dp', None), P(), P(None, 'dp'))
    n_dev = mesh.shape['dp']

    def device_step(hidden, lengths, kv_cache, norm_attn, w_q, w_o, norm_ffn, w_gate, w_up, w_down, norm_final, w_head):
        gathered = decode_layers(n_dev, lengths, hidden, kv_cache, norm_attn, w_q, w_o, norm_ffn, w_gate, w_up, w_down,
                                 norm_final)
        return jnp.dot(gathered, w_head, preferred_element_type=jnp.float32)

    return jax.shard_map(device_step, mesh=mesh, in_specs=specs_in, out_specs=P('rep', 'dp'), check_vma=False)
```

```python
import functools

import jax
import jax.numpy as jnp
from jax import lax
from jax.experimental import pallas as pl
from jax.experimental.pallas import tpu as pltpu
from jax.sharding import PartitionSpec as P

LATENT_DIM = 512
QK_SCALE = 192 ** -0.5
NORM_EPS = 1e-6
MESH = pl.DeviceIdType.MESH
BF16, F32 = jnp.bfloat16, jnp.float32
TILE = 256
LANES = 128
AG_LAG = 2
AG_STRAIGHT = 2
RS_LAG = 2
GROUP = 8


def rms_norm(x_float, gain_row):
    inv_rms = lax.rsqrt(jnp.mean(x_float * x_float, axis=-1, keepdims=True) + NORM_EPS)
    return (x_float * inv_rms * gain_row).astype(BF16)


def decode_kernel(cfg, lengths, hidden, kv_hbm, norm_attn, wq_hbm, wo_hbm, norm_ffn, wg_hbm, wu_hbm, wd_hbm, norm_final,
                  w_head_hbm, out, wa, kv_b, x_full, h_s, q_s, o_s, o_all, xg, act, y_send, y_recv, y_sum, relay_in, relay_out,
                  direct_in, w_sem, kv_sem, head_sem, x_send, x_recv, q_send, q_recv, o_send, o_recv, ag_send, ag_recv,
                  d2d_send, d2d_recv, y_ssem, y_rsem, rs_send, rs_recv):
    num_layers, rows, heads, width, d_model, ffn, n_dev = cfg
    chips = n_dev // 2
    pair = 2 * rows
    half_d = d_model // 2
    half_h = heads // 2
    q_cols = half_h * width
    t_tiles = half_d // TILE
    q_parts = q_s.shape[0]

    me = lax.axis_index("dp")
    chip, core = lax.div(me, 2), lax.rem(me, 2)
    other = 1 - core
    partner = chip * 2 + other
    right_chip, left_chip = lax.rem(chip + 1, chips), lax.rem(chip + chips - 1, chips)
    far_chip = lax.rem(chip + 2, chips)
    right, left, far = right_chip * 2 + core, left_chip * 2 + core, far_chip * 2 + core

    def remote(src, dst, send_sem, recv_sem, device):
        return pltpu.make_async_remote_copy(src_ref=src, dst_ref=dst, send_sem=send_sem, recv_sem=recv_sem,
                                            device_id={"dp": device}, device_id_type=MESH)

    pair_cols = 2 * width
    n_q = q_cols // pair_cols
    o_depth = d_model
    n_o = wo_hbm.shape[1] // o_depth
    wo_base = wa.shape[1] - n_o * half_d
    kv_parts = rows // GROUP

    def q_copy(l, p):
        col = pl.multiple_of(core * q_cols + p * pair_cols, LANES)
        return pltpu.make_async_copy(wq_hbm.at[l, :, pl.ds(col, pair_cols)],
                                     wa.at[:, p * pair_cols:(p + 1) * pair_cols], w_sem.at[p])

    def o_copy(l, p):
        col = pl.multiple_of(core * half_d, LANES)
        return pltpu.make_async_copy(wo_hbm.at[l, p * o_depth:(p + 1) * o_depth, pl.ds(col, half_d)],
                                     wa.at[:, wo_base + p * half_d:wo_base + (p + 1) * half_d], w_sem.at[n_q + p])

    def ffn_copies(l):
        return [pltpu.make_async_copy(wg_hbm.at[l], wa.at[:, 0:ffn], w_sem.at[n_q + n_o]),
                pltpu.make_async_copy(wu_hbm.at[l], wa.at[:, ffn:2 * ffn], w_sem.at[n_q + n_o + 1]),
                pltpu.make_async_copy(wd_hbm.at[l], wa.at[0:ffn, 2 * ffn:2 * ffn + d_model], w_sem.at[n_q + n_o + 2])]

    def head_copy(which):
        cols = (slice(wo_base, wa.shape[1]), slice(0, wo_base))[which]
        return pltpu.make_async_copy(w_head_hbm.at[:, cols], wa.at[:, cols], head_sem.at[which])

    def kv_copy(l, g):
        return pltpu.make_async_copy(kv_hbm.at[l, g * GROUP:(g + 1) * GROUP],
                                     kv_b.at[g * GROUP:(g + 1) * GROUP], kv_sem.at[g])

    for p in range(n_q):
        q_copy(0, p).start()
    for g in range(kv_parts):
        kv_copy(0, g).start()
    for p in range(n_o):
        o_copy(0, p).start()

    barrier = pltpu.get_barrier_semaphore()
    for device in (partner, left, right, far):
        pl.semaphore_signal(barrier, inc=1, device_id={"dp": device}, device_id_type=MESH)
    pl.semaphore_wait(barrier, 4)

    if width % LANES:
        q_s[q_parts - 1] = jnp.zeros(q_s.shape[1:], F32)

    own_rows = pl.ds(pl.multiple_of(core * rows, rows), rows)
    first = remote(hidden, x_full.at[own_rows, :], x_send.at[0], x_recv.at[0], partner)
    first.start()
    x_full[own_rows, :] = hidden[...]
    first.wait()

    def half_cols(which, t=0, n=None):
        return pl.ds(pl.multiple_of(which * half_d + t * TILE, LANES), half_d if n is None else n)

    def rows_of(which_chip, half, count=rows):
        return pl.ds(pl.multiple_of(which_chip * pair + half * rows, rows), count)

    ring_pieces = ((chip, 0, right), (chip, 1, left), (chip, 1, right), (chip, 0, left), (left_chip, 0, right), (right_chip, 1, left),
                   (chip, 0, far), (chip, 1, far))
    pair_pieces = ((chip, 0), (left_chip, 0), (right_chip, 1), (left_chip, 1), (right_chip, 0), (far_chip, 0), (far_chip, 1))

    def ring_copy(slot, t):
        which_chip, half, device = ring_pieces[slot]
        at = xg.at[rows_of(which_chip, half), half_cols(core, t, TILE)]
        slot = slot - 2 if slot >= 6 else slot
        return remote(at, at, ag_send.at[slot, t], ag_recv.at[slot, t], device)

    def pair_copy(slot, t):
        which_chip, half = pair_pieces[slot]
        at = xg.at[rows_of(which_chip, half, rows if slot else pair), half_cols(core, t, TILE)]
        return remote(at, at, d2d_send.at[slot, t], d2d_recv.at[slot, t], partner)

    def gather_start(t):
        def straight():
            ring_copy(6, t).start()
            ring_copy(7, t).start()

        if isinstance(t, int):
            if t >= AG_STRAIGHT:
                straight()
        else:
            pl.when(t >= AG_STRAIGHT)(straight)
        for slot in range(4):
            ring_copy(slot, t).start()
        pair_copy(0, t).start()

    def gather_near(t):
        for slot in range(4):
            ring_copy(slot, t).wait_recv()
            if slot < 2 and t < AG_STRAIGHT:
                ring_copy(4 + slot, t).start()
            pair_copy(1 + slot, t).start()

    def gather_end(first, gain_row, dst):
        def arrived(slots, which_chip):
            for slot in slots:
                for t in range(t_tiles):
                    pair_copy(slot, t).wait_recv()
            at = pl.ds(pl.multiple_of(which_chip * pair, pair), pair)
            dst[at, :] = rms_norm(xg[at, :].astype(F32), gain_row)

        def gather_far(t):
            for slot in range(2):
                ring_copy(4 + slot, t).wait_recv()
                pair_copy(5 + slot, t).start()

        for t in range(first, t_tiles - 1):
            gather_near(t)
        arrived((0,), chip)
        gather_near(t_tiles - 1)
        for t in range(AG_STRAIGHT):
            gather_far(t)
        arrived((1, 3), left_chip)
        arrived((2, 4), right_chip)
        for t in range(AG_STRAIGHT, t_tiles):
            gather_far(t)
        arrived((5, 6), far_chip)
        for t in range(t_tiles):
            for slot in range(4):
                ring_copy(slot, t).wait_send()
            for slot in range(2):
                ring_copy((6 if t >= AG_STRAIGHT else 4) + slot, t).wait_send()
            for slot in range(7):
                pair_copy(slot, t).wait_send()

    own_chip_rows = pl.ds(pl.multiple_of(chip * pair, pair), pair)

    for layer in range(num_layers):
        h_s[...] = rms_norm(x_full[...].astype(F32), norm_attn[layer:layer + 1, :])
        q_copies = []
        for p in range(n_q):
            q_copy(layer, p).wait()
            q_val = jnp.dot(h_s[...], wa[:, p * pair_cols:(p + 1) * pair_cols], preferred_element_type=F32)
            q_val = q_val.astype(BF16).astype(F32)
            for e in range(2):
                head = core * half_h + 2 * p + e
                base = pl.multiple_of(head * pair, pair)
                q_head = q_val[:, e * width:(e + 1) * width]
                for c in range(q_parts):
                    lanes = min(LANES, width - c * LANES)
                    q_s[c, pl.ds(base, pair), 0:lanes] = q_head[:, c * LANES:c * LANES + lanes]
                away = pl.ds(pl.multiple_of(base + other * rows, rows), rows)
                copy = remote(q_s.at[:, away, :], q_s.at[:, away, :], q_send.at[2 * p + e], q_recv.at[2 * p + e], partner)
                copy.start()
                q_copies.append(copy)
        for copy in ffn_copies(layer):
            copy.start()
        for copy in q_copies:
            copy.wait_recv()

        o_copies = []
        per_half = kv_parts // 2
        key_pos = lax.broadcasted_iota(jnp.int32, (heads, kv_b.shape[2]), 1)
        for half in range(2):
            for g in range(half * per_half, (half + 1) * per_half):
                kv_copy(layer, g).wait()
                scores = []
                for i in range(GROUP):
                    b = g * GROUP + i
                    at = pl.ds(core * rows + b, heads, stride=pair)
                    q_b = jnp.concatenate([q_s[c, at, :] for c in range(q_parts)], axis=1)[:, 0:width].astype(BF16)
                    s_b = jnp.dot(q_b, kv_b[b], preferred_element_type=F32) * QK_SCALE
                    scores.append(jnp.where(key_pos < lengths[b], s_b, -1e30))
                s_all = jnp.concatenate(scores, axis=0)
                e_all = jnp.exp(s_all - jnp.max(s_all, axis=-1, keepdims=True))
                p_all = (e_all / jnp.sum(e_all, axis=-1, keepdims=True)).astype(BF16)
                for i in range(GROUP):
                    b = g * GROUP + i
                    o_b = lax.dot_general(p_all[i * heads:(i + 1) * heads, :], kv_b[b, 0:LATENT_DIM, :],
                                          (((1,), (1,)), ((), ())), preferred_element_type=F32)
                    for c in range(LATENT_DIM // LANES):
                        o_s[c, pl.ds(b, heads, stride=rows), :] = o_b[:, c * LANES:(c + 1) * LANES]
                if layer + 1 < num_layers:
                    kv_copy(layer + 1, g).start()
            part = rows // 2
            at = pl.ds(pl.multiple_of(core * rows + half * part, part), part)
            for head in range(heads):
                for c in range(LATENT_DIM // LANES):
                    o_all[at, head * LATENT_DIM + c * LANES:head * LATENT_DIM + (c + 1) * LANES] = \
                        o_s[c, head * rows + half * part:head * rows + (half + 1) * part, :].astype(BF16)
            copy = remote(o_all.at[at, :], o_all.at[at, :], o_send.at[half], o_recv.at[half], partner)
            copy.start()
            o_copies.append(copy)
        for copy in q_copies:
            copy.wait_send()

        for p in range(n_o):
            o_copy(layer, p).wait()
        for copy in o_copies:
            copy.wait_recv()

        def wo_tile(t, carry):
            o_val = jnp.zeros((pair, TILE), F32)
            for p in range(n_o):
                cols = pl.ds(pl.multiple_of(wo_base + p * half_d + t * TILE, LANES), TILE)
                o_val += jnp.dot(o_all[:, p * o_depth:(p + 1) * o_depth], wa[:, cols], preferred_element_type=F32)
            xg[own_chip_rows, half_cols(core, t, TILE)] = \
                (x_full[:, half_cols(core, t, TILE)].astype(F32) + o_val).astype(BF16)
            gather_start(t)
            return carry

        lax.fori_loop(0, t_tiles, wo_tile, 0)
        for copy in o_copies:
            copy.wait_send()
        if layer + 1 < num_layers:
            for p in range(n_o):
                o_copy(layer + 1, p).start()
        else:
            head_copy(0).start()

        gather_end(0, norm_ffn[layer:layer + 1, :], out)
        for copy in ffn_copies(layer):
            copy.wait()

        for j in range(0, ffn, LANES):
            both = jnp.concatenate([wa[:, j:j + LANES], wa[:, ffn + j:ffn + j + LANES]], axis=1)
            val = jnp.dot(out[...], both, preferred_element_type=F32)
            act[:, j:j + LANES] = (jax.nn.silu(val[:, :LANES]) * val[:, LANES:]).astype(BF16)

        def down(which, t):
            cols = pl.ds(pl.multiple_of(2 * ffn + which * half_d + t * TILE, LANES), TILE)
            return jnp.dot(act[...], wa[0:ffn, cols], preferred_element_type=F32)

        y_copies = []
        def away(t):
            y_send[t] = down(other, t)
            copy = remote(y_send.at[t], y_recv.at[t], y_ssem.at[t], y_rsem.at[t], partner)
            copy.start()
            y_copies.append(copy)

        def rs_copy(src, dst, slot, t, device):
            copy = remote(src, dst, rs_send.at[slot, t], rs_recv.at[slot, t], device)
            copy.start()
            return copy

        rs_relay, rs_direct, rs_final = [], [], []

        def relay(t):
            for d, device, target in ((0, right, right_chip), (1, left, left_chip)):
                rs_relay[t][d].wait_recv()
                relay_out[d, t] = relay_in[d, t] + y_sum[t, rows_of(target, d), :]
                rs_final[t].append(rs_copy(relay_out.at[d, t], direct_in.at[2 + d, t], 4 + d, t, device))

        def own(t):
            val = down(core, t)
            y_copies[t].wait_recv()
            y_sum[t] = val + y_recv[t]
            rs_relay.append([rs_copy(y_sum.at[t, rows_of(far_chip, 0), :], relay_in.at[0, t], 0, t, right),
                             rs_copy(y_sum.at[t, rows_of(far_chip, 1), :], relay_in.at[1, t], 1, t, left)])
            rs_direct.append([rs_copy(y_sum.at[t, rows_of(right_chip, 1), :], direct_in.at[0, t], 2, t, right),
                              rs_copy(y_sum.at[t, rows_of(left_chip, 0), :], direct_in.at[1, t], 3, t, left)])
            rs_final.append([])

        away(0)
        for t in range(t_tiles):
            if t + 1 < t_tiles:
                away(t + 1)
            own(t)
            if t >= RS_LAG:
                relay(t - RS_LAG)
        for t in range(t_tiles - RS_LAG, t_tiles):
            relay(t)
        if layer + 1 < num_layers:
            for p in range(n_q):
                q_copy(layer + 1, p).start()
        else:
            head_copy(1).start()

        last = layer + 1 == num_layers
        x_copies = []
        for t in range(t_tiles):
            for copy in rs_direct[t] + rs_final[t]:
                copy.wait_recv()
            cols = half_cols(core, t, TILE)
            for half in range(2):
                total = (y_sum[t, rows_of(chip, half), :] + direct_in[2 + half, t]) + direct_in[1 - half, t]
                x_new = (xg[rows_of(chip, half), cols].astype(F32) + total).astype(BF16)
                if last:
                    xg[rows_of(chip, half), cols] = x_new
                else:
                    x_full[half * rows:(half + 1) * rows, cols] = x_new
            if last:
                gather_start(t)
                if t >= AG_LAG:
                    gather_near(t - AG_LAG)
            else:
                copy = remote(x_full.at[:, cols], x_full.at[:, cols], x_send.at[1 + t], x_recv.at[1 + t], partner)
                copy.start()
                x_copies.append(copy)
        for copy in y_copies:
            copy.wait_send()
        for group in rs_relay + rs_direct + rs_final:
            for copy in group:
                copy.wait_send()
        for copy in x_copies:
            copy.wait()

    gather_end(t_tiles - AG_LAG, norm_final[0:1, :], out)
    head_copy(0).wait()
    head_copy(1).wait()


def head_kernel(h_ref, ahead, w_hbm, out_hbm, ring, stage, w_sem, out_sem):
    slots, _, tile = ring.shape
    n_stage = stage.shape[0]
    n_ahead = ahead.shape[1] // tile
    n_stream = w_hbm.shape[1] // tile - n_ahead

    def col(t):
        return pl.ds(pl.multiple_of(t * tile, tile), tile)

    def fetch(i, slot):
        return pltpu.make_async_copy(w_hbm.at[:, col(n_ahead + i)], ring.at[slot], w_sem.at[slot])

    def put(t, slot):
        return pltpu.make_async_copy(stage.at[slot], out_hbm.at[:, col(t)], out_sem.at[slot])

    for i in range(slots):
        fetch(i, i).start()

    def tiles(n, jobs):
        for e, _ in enumerate(jobs):
            @pl.when(n + e >= n_stage)
            def _():
                put(0, lax.rem(n + e, n_stage)).wait()
        for e, (t, weights) in enumerate(jobs):
            for c in range(0, tile, TILE):
                stage[lax.rem(n + e, n_stage), :, c:c + TILE] = \
                    jnp.dot(h_ref[...], weights(c), preferred_element_type=F32)
        for e, (t, weights) in enumerate(jobs):
            put(t, lax.rem(n + e, n_stage)).start()

    def from_ahead(i):
        return i, lambda c: ahead[:, pl.ds(pl.multiple_of(i * tile + c, TILE), TILE)]

    def from_ring(i):
        return n_ahead + i, lambda c: ring[lax.rem(i, slots), :, c:c + TILE]

    def refill(i):
        @pl.when(i + slots < n_stream)
        def _():
            fetch(i + slots, lax.rem(i, slots)).start()

    n_both = n_ahead - 2

    def both(i, carry):
        fetch(i, lax.rem(i, slots)).wait()
        tiles(2 * i + 2, [from_ahead(i + 2), from_ring(i)])
        refill(i)
        return carry

    def alone(j, carry):
        i = n_both + 2 * j
        for e in range(2):
            fetch(i + e, lax.rem(i + e, slots)).wait()
        tiles(n_ahead + i, [from_ring(i), from_ring(i + 1)])
        for e in range(2):
            refill(i + e)
        return carry

    tiles(0, [from_ahead(0), from_ahead(1)])
    lax.fori_loop(0, n_both, both, 0)
    lax.fori_loop(0, (n_stream - n_both) // 2, alone, 0)
    for s in range(n_stage):
        put(0, s).wait()


def head_matmul(gathered, ahead, w_head):
    tile, slots, n_stage = 1024, 3, 4
    depth, cols = w_head.shape
    rows = gathered.shape[0]
    hbm, vmem = pl.BlockSpec(memory_space=pl.ANY), pl.BlockSpec(memory_space=pltpu.VMEM)
    return pl.pallas_call(
        head_kernel,
        out_shape=jax.ShapeDtypeStruct((rows, cols), F32),
        in_specs=[vmem, vmem, hbm],
        out_specs=hbm,
        scratch_shapes=[pltpu.VMEM((slots, depth, tile), BF16), pltpu.VMEM((n_stage, rows, tile), F32),
                        pltpu.SemaphoreType.DMA((slots,)), pltpu.SemaphoreType.DMA((n_stage,))],
        compiler_params=pltpu.CompilerParams(vmem_limit_bytes=22 * 1024 * 1024),
        cost_estimate=pl.CostEstimate(flops=2 * rows * depth * cols, bytes_accessed=2 * depth * cols + 4 * rows * cols,
                                      transcendentals=0),
        name="head_matmul",
    )(gathered, ahead, w_head)


def decode_layers(n_dev, lengths, hidden, kv_cache, norm_attn, w_q, w_o, norm_ffn, w_gate, w_up, w_down, norm_final, w_head):
    num_layers, rows, seq_len, width = kv_cache.shape
    d_model = hidden.shape[1]
    heads = w_q.shape[2] // width
    ffn = w_gate.shape[2]
    pair, group_rows, half_d = 2 * rows, n_dev * rows, d_model // 2
    q_cols = heads * width // 2
    wa_cols = max(q_cols, 2 * ffn + d_model)
    wa_cols = -(-wa_cols // LANES) * LANES
    t_tiles = half_d // TILE
    pad_width = -(-width // LANES) * LANES
    hbm, vmem = pl.BlockSpec(memory_space=pl.ANY), pl.BlockSpec(memory_space=pltpu.VMEM)
    smem = pl.BlockSpec(memory_space=pltpu.SMEM)
    dma = pltpu.SemaphoreType.DMA
    cfg = (num_layers, rows, heads, width, d_model, ffn, n_dev)
    n_q = q_cols // (2 * width)
    scratch = [
        pltpu.VMEM((rows, width, seq_len), BF16),
        pltpu.VMEM((pair, d_model), BF16),
        pltpu.VMEM((pair, d_model), BF16),
        pltpu.VMEM((pad_width // LANES, heads * pair, LANES), F32),
        pltpu.VMEM((LATENT_DIM // LANES, heads * rows, LANES), F32),
        pltpu.VMEM((pair, heads * LATENT_DIM), BF16),
        pltpu.VMEM((group_rows, d_model), BF16),
        pltpu.VMEM((group_rows, ffn), BF16),
        pltpu.VMEM((t_tiles, group_rows, TILE), F32),
        pltpu.VMEM((t_tiles, group_rows, TILE), F32),
        pltpu.VMEM((t_tiles, group_rows, TILE), F32),
        pltpu.VMEM((2, t_tiles, rows, TILE), F32),
        pltpu.VMEM((2, t_tiles, rows, TILE), F32),
        pltpu.VMEM((4, t_tiles, rows, TILE), F32),
        dma((n_q + 4 + 3,)),
        dma((rows // GROUP,)),
        dma((2,)),
        dma((1 + t_tiles,)), dma((1 + t_tiles,)),
        dma((2 * n_q,)), dma((2 * n_q,)),
        dma((2,)), dma((2,)),
        dma((6, t_tiles)), dma((6, t_tiles)),
        dma((7, t_tiles)), dma((7, t_tiles)),
        dma((t_tiles,)), dma((t_tiles,)),
        dma((6, t_tiles)), dma((6, t_tiles)),
    ]
    gathered, ahead = pl.pallas_call(
        functools.partial(decode_kernel, cfg),
        out_shape=(pltpu.VMEM((group_rows, d_model), BF16), pltpu.VMEM((d_model, wa_cols + w_o.shape[1] // d_model * half_d), BF16)),
        in_specs=[smem, vmem, hbm, vmem, hbm, hbm, vmem, hbm, hbm, hbm, vmem, hbm],
        out_specs=(vmem, vmem),
        scratch_shapes=scratch,
        compiler_params=pltpu.CompilerParams(collective_id=0, has_side_effects=True, vmem_limit_bytes=26 * 1024 * 1024),
        name="decode_layers",
    )(lengths, hidden, jnp.swapaxes(kv_cache, 2, 3), norm_attn, w_q, w_o, norm_ffn, w_gate, w_up, w_down, norm_final.reshape(1, -1), w_head)
    gathered, ahead = (pltpu.with_memory_space_constraint(a, pltpu.VMEM) for a in (gathered, ahead))
    return head_matmul(gathered, ahead, w_head)


def solution(mesh):
    row_axes = ('rep', 'dp')
    specs_in = (P(row_axes, None), P(row_axes), P(None, row_axes, None, None), P(), P(), P(), P(),
                P(None, None, 'dp'), P(None, None, 'dp'), P(None, 'dp', None), P(), P(None, 'dp'))
    n_dev = mesh.shape['dp']

    def device_step(hidden, lengths, kv_cache, norm_attn, w_q, w_o, norm_ffn, w_gate, w_up, w_down, norm_final, w_head):
        return decode_layers(n_dev, lengths, hidden, kv_cache, norm_attn, w_q, w_o, norm_ffn, w_gate, w_up, w_down,
                             norm_final, w_head)

    return jax.shard_map(device_step, mesh=mesh, in_specs=specs_in, out_specs=P('rep', 'dp'), check_vma=False)
```

```python
import functools

import jax
import jax.numpy as jnp
from jax import lax
from jax.experimental import pallas as pl
from jax.experimental.pallas import tpu as pltpu
from jax.sharding import PartitionSpec as P

LATENT_DIM = 512
QK_SCALE = 192 ** -0.5
NORM_EPS = 1e-6
MESH = pl.DeviceIdType.MESH
BF16, F32 = jnp.bfloat16, jnp.float32
TILE = 256
LANES = 128
AG_LAG = 2
AG_STRAIGHT = 2
RS_LAG = 2
GROUP = 8


def rms_norm(x_float, gain_row):
    inv_rms = lax.rsqrt(jnp.mean(x_float * x_float, axis=-1, keepdims=True) + NORM_EPS)
    return (x_float * inv_rms * gain_row).astype(BF16)


def decode_kernel(cfg, lengths, hidden, kv_hbm, norm_attn, wq_hbm, wo_hbm, norm_ffn, wg_hbm, wu_hbm, wd_hbm, norm_final,
                  w_head_hbm, out, wa, kv_b, x_full, h_s, q_s, o_s, o_all, xg, act, y_send, y_recv, y_sum, relay_in, relay_out,
                  direct_in, w_sem, kv_sem, head_sem, x_send, x_recv, q_send, q_recv, o_send, o_recv, ag_send, ag_recv,
                  d2d_send, d2d_recv, y_ssem, y_rsem, rs_send, rs_recv):
    num_layers, rows, heads, width, d_model, ffn, n_dev = cfg
    chips = n_dev // 2
    pair = 2 * rows
    half_d = d_model // 2
    half_h = heads // 2
    q_cols = half_h * width
    t_tiles = half_d // TILE
    q_parts = q_s.shape[0]

    me = lax.axis_index("dp")
    chip, core = lax.div(me, 2), lax.rem(me, 2)
    other = 1 - core
    partner = chip * 2 + other
    right_chip, left_chip = lax.rem(chip + 1, chips), lax.rem(chip + chips - 1, chips)
    far_chip = lax.rem(chip + 2, chips)
    right, left, far = right_chip * 2 + core, left_chip * 2 + core, far_chip * 2 + core

    def remote(src, dst, send_sem, recv_sem, device):
        return pltpu.make_async_remote_copy(src_ref=src, dst_ref=dst, send_sem=send_sem, recv_sem=recv_sem,
                                            device_id={"dp": device}, device_id_type=MESH)

    pair_cols = 2 * width
    n_q = q_cols // pair_cols
    o_depth = d_model
    n_o = wo_hbm.shape[1] // o_depth
    wo_base = wa.shape[1] - n_o * half_d
    kv_parts = rows // GROUP

    def q_copy(l, p):
        col = pl.multiple_of(core * q_cols + p * pair_cols, LANES)
        return pltpu.make_async_copy(wq_hbm.at[l, :, pl.ds(col, pair_cols)],
                                     wa.at[:, p * pair_cols:(p + 1) * pair_cols], w_sem.at[p])

    def o_copy(l, p):
        col = pl.multiple_of(core * half_d, LANES)
        return pltpu.make_async_copy(wo_hbm.at[l, p * o_depth:(p + 1) * o_depth, pl.ds(col, half_d)],
                                     wa.at[:, wo_base + p * half_d:wo_base + (p + 1) * half_d], w_sem.at[n_q + p])

    def ffn_copies(l):
        return [pltpu.make_async_copy(wg_hbm.at[l], wa.at[:, 0:ffn], w_sem.at[n_q + n_o]),
                pltpu.make_async_copy(wu_hbm.at[l], wa.at[:, ffn:2 * ffn], w_sem.at[n_q + n_o + 1]),
                pltpu.make_async_copy(wd_hbm.at[l], wa.at[0:ffn, 2 * ffn:2 * ffn + d_model], w_sem.at[n_q + n_o + 2])]

    def head_copy(which):
        cols = (slice(wo_base, wa.shape[1]), slice(0, wo_base))[which]
        return pltpu.make_async_copy(w_head_hbm.at[:, cols], wa.at[:, cols], head_sem.at[which])

    def kv_copy(l, g):
        return pltpu.make_async_copy(kv_hbm.at[l, g * GROUP:(g + 1) * GROUP],
                                     kv_b.at[g * GROUP:(g + 1) * GROUP], kv_sem.at[g])

    for p in range(n_q):
        q_copy(0, p).start()
    for g in range(kv_parts):
        kv_copy(0, g).start()
    for p in range(n_o):
        o_copy(0, p).start()

    barrier = pltpu.get_barrier_semaphore()
    for device in (partner, left, right, far):
        pl.semaphore_signal(barrier, inc=1, device_id={"dp": device}, device_id_type=MESH)
    pl.semaphore_wait(barrier, 4)

    if width % LANES:
        q_s[q_parts - 1] = jnp.zeros(q_s.shape[1:], F32)

    own_rows = pl.ds(pl.multiple_of(core * rows, rows), rows)
    first = remote(hidden, x_full.at[own_rows, :], x_send.at[0], x_recv.at[0], partner)
    first.start()
    x_full[own_rows, :] = hidden[...]
    first.wait()

    def half_cols(which, t=0, n=None):
        return pl.ds(pl.multiple_of(which * half_d + t * TILE, LANES), half_d if n is None else n)

    def rows_of(which_chip, half, count=rows):
        return pl.ds(pl.multiple_of(which_chip * pair + half * rows, rows), count)

    ring_pieces = ((chip, 0, right), (chip, 1, left), (chip, 1, right), (chip, 0, left), (left_chip, 0, right), (right_chip, 1, left),
                   (chip, 0, far), (chip, 1, far))
    pair_pieces = ((chip, 0), (left_chip, 0), (right_chip, 1), (left_chip, 1), (right_chip, 0), (far_chip, 0), (far_chip, 1))

    def ring_copy(slot, t):
        which_chip, half, device = ring_pieces[slot]
        at = xg.at[rows_of(which_chip, half), half_cols(core, t, TILE)]
        slot = slot - 2 if slot >= 6 else slot
        return remote(at, at, ag_send.at[slot, t], ag_recv.at[slot, t], device)

    def pair_copy(slot, t):
        which_chip, half = pair_pieces[slot]
        at = xg.at[rows_of(which_chip, half, rows if slot else pair), half_cols(core, t, TILE)]
        return remote(at, at, d2d_send.at[slot, t], d2d_recv.at[slot, t], partner)

    def gather_start(t):
        def straight():
            ring_copy(6, t).start()
            ring_copy(7, t).start()

        if isinstance(t, int):
            if t >= AG_STRAIGHT:
                straight()
        else:
            pl.when(t >= AG_STRAIGHT)(straight)
        for slot in range(4):
            ring_copy(slot, t).start()
        pair_copy(0, t).start()

    def gather_near(t):
        for slot in range(4):
            ring_copy(slot, t).wait_recv()
            if slot < 2 and t < AG_STRAIGHT:
                ring_copy(4 + slot, t).start()
            pair_copy(1 + slot, t).start()

    def gather_end(first, gain_row, dst):
        def arrived(slots, which_chip):
            for slot in slots:
                for t in range(t_tiles):
                    pair_copy(slot, t).wait_recv()
            at = pl.ds(pl.multiple_of(which_chip * pair, pair), pair)
            dst[at, :] = rms_norm(xg[at, :].astype(F32), gain_row)

        def gather_far(t):
            for slot in range(2):
                ring_copy(4 + slot, t).wait_recv()
                pair_copy(5 + slot, t).start()

        for t in range(first, t_tiles - 1):
            gather_near(t)
        arrived((0,), chip)
        gather_near(t_tiles - 1)
        for t in range(AG_STRAIGHT):
            gather_far(t)
        arrived((1, 3), left_chip)
        arrived((2, 4), right_chip)
        for t in range(AG_STRAIGHT, t_tiles):
            gather_far(t)
        arrived((5, 6), far_chip)
        for t in range(t_tiles):
            for slot in range(4):
                ring_copy(slot, t).wait_send()
            for slot in range(2):
                ring_copy((6 if t >= AG_STRAIGHT else 4) + slot, t).wait_send()
            for slot in range(7):
                pair_copy(slot, t).wait_send()

    own_chip_rows = pl.ds(pl.multiple_of(chip * pair, pair), pair)

    for layer in range(num_layers):
        h_s[...] = rms_norm(x_full[...].astype(F32), norm_attn[layer:layer + 1, :])
        q_copies = []
        for p in range(n_q):
            q_copy(layer, p).wait()
            q_val = jnp.dot(h_s[...], wa[:, p * pair_cols:(p + 1) * pair_cols], preferred_element_type=F32)
            q_val = q_val.astype(BF16).astype(F32)
            for e in range(2):
                head = core * half_h + 2 * p + e
                base = pl.multiple_of(head * pair, pair)
                q_head = q_val[:, e * width:(e + 1) * width]
                for c in range(q_parts):
                    lanes = min(LANES, width - c * LANES)
                    q_s[c, pl.ds(base, pair), 0:lanes] = q_head[:, c * LANES:c * LANES + lanes]
                away = pl.ds(pl.multiple_of(base + other * rows, rows), rows)
                copy = remote(q_s.at[:, away, :], q_s.at[:, away, :], q_send.at[2 * p + e], q_recv.at[2 * p + e], partner)
                copy.start()
                q_copies.append(copy)
        for copy in ffn_copies(layer):
            copy.start()
        for copy in q_copies:
            copy.wait_recv()

        o_copies = []
        per_half = kv_parts // 2
        key_pos = lax.broadcasted_iota(jnp.int32, (heads, kv_b.shape[2]), 1)
        for half in range(2):
            for g in range(half * per_half, (half + 1) * per_half):
                kv_copy(layer, g).wait()
                scores = []
                for i in range(GROUP):
                    b = g * GROUP + i
                    at = pl.ds(core * rows + b, heads, stride=pair)
                    q_b = jnp.concatenate([q_s[c, at, :] for c in range(q_parts)], axis=1)[:, 0:width].astype(BF16)
                    s_b = jnp.dot(q_b, kv_b[b], preferred_element_type=F32) * QK_SCALE
                    scores.append(jnp.where(key_pos < lengths[b], s_b, -1e30))
                s_all = jnp.concatenate(scores, axis=0)
                e_all = jnp.exp(s_all - jnp.max(s_all, axis=-1, keepdims=True))
                p_all = (e_all / jnp.sum(e_all, axis=-1, keepdims=True)).astype(BF16)
                for i in range(GROUP):
                    b = g * GROUP + i
                    o_b = lax.dot_general(p_all[i * heads:(i + 1) * heads, :], kv_b[b, 0:LATENT_DIM, :],
                                          (((1,), (1,)), ((), ())), preferred_element_type=F32)
                    for c in range(LATENT_DIM // LANES):
                        o_s[c, pl.ds(b, heads, stride=rows), :] = o_b[:, c * LANES:(c + 1) * LANES]
                if layer + 1 < num_layers:
                    kv_copy(layer + 1, g).start()
            part = rows // 2
            at = pl.ds(pl.multiple_of(core * rows + half * part, part), part)
            for head in range(heads):
                for c in range(LATENT_DIM // LANES):
                    o_all[at, head * LATENT_DIM + c * LANES:head * LATENT_DIM + (c + 1) * LANES] = \
                        o_s[c, head * rows + half * part:head * rows + (half + 1) * part, :].astype(BF16)
            copy = remote(o_all.at[at, :], o_all.at[at, :], o_send.at[half], o_recv.at[half], partner)
            copy.start()
            o_copies.append(copy)
        for copy in q_copies:
            copy.wait_send()

        for p in range(n_o):
            o_copy(layer, p).wait()
        for copy in o_copies:
            copy.wait_recv()

        def wo_tile(t, carry):
            o_val = jnp.zeros((pair, TILE), F32)
            for p in range(n_o):
                cols = pl.ds(pl.multiple_of(wo_base + p * half_d + t * TILE, LANES), TILE)
                o_val += jnp.dot(o_all[:, p * o_depth:(p + 1) * o_depth], wa[:, cols], preferred_element_type=F32)
            xg[own_chip_rows, half_cols(core, t, TILE)] = \
                (x_full[:, half_cols(core, t, TILE)].astype(F32) + o_val).astype(BF16)
            gather_start(t)
            return carry

        lax.fori_loop(0, t_tiles, wo_tile, 0)
        for copy in o_copies:
            copy.wait_send()
        if layer + 1 < num_layers:
            for p in range(n_o):
                o_copy(layer + 1, p).start()
        else:
            head_copy(0).start()

        gather_end(0, norm_ffn[layer:layer + 1, :], out)
        for copy in ffn_copies(layer):
            copy.wait()

        for j in range(0, ffn, LANES):
            both = jnp.concatenate([wa[:, j:j + LANES], wa[:, ffn + j:ffn + j + LANES]], axis=1)
            val = jnp.dot(out[...], both, preferred_element_type=F32)
            act[:, j:j + LANES] = (jax.nn.silu(val[:, :LANES]) * val[:, LANES:]).astype(BF16)

        def down(which, t):
            cols = pl.ds(pl.multiple_of(2 * ffn + which * half_d + t * TILE, LANES), TILE)
            return jnp.dot(act[...], wa[0:ffn, cols], preferred_element_type=F32)

        y_copies = []
        def away(t):
            y_send[t] = down(other, t)
            copy = remote(y_send.at[t], y_recv.at[t], y_ssem.at[t], y_rsem.at[t], partner)
            copy.start()
            y_copies.append(copy)

        def rs_copy(src, dst, slot, t, device):
            copy = remote(src, dst, rs_send.at[slot, t], rs_recv.at[slot, t], device)
            copy.start()
            return copy

        rs_relay, rs_direct, rs_final = [], [], []

        def relay(t):
            for d, device, target in ((0, right, right_chip), (1, left, left_chip)):
                rs_relay[t][d].wait_recv()
                relay_out[d, t] = relay_in[d, t] + y_sum[t, rows_of(target, d), :]
                rs_final[t].append(rs_copy(relay_out.at[d, t], direct_in.at[2 + d, t], 4 + d, t, device))

        def own(t):
            val = down(core, t)
            y_copies[t].wait_recv()
            y_sum[t] = val + y_recv[t]
            rs_relay.append([rs_copy(y_sum.at[t, rows_of(far_chip, 0), :], relay_in.at[0, t], 0, t, right),
                             rs_copy(y_sum.at[t, rows_of(far_chip, 1), :], relay_in.at[1, t], 1, t, left)])
            rs_direct.append([rs_copy(y_sum.at[t, rows_of(right_chip, 1), :], direct_in.at[0, t], 2, t, right),
                              rs_copy(y_sum.at[t, rows_of(left_chip, 0), :], direct_in.at[1, t], 3, t, left)])
            rs_final.append([])

        away(0)
        for t in range(t_tiles):
            if t + 1 < t_tiles:
                away(t + 1)
            own(t)
            if t >= RS_LAG:
                relay(t - RS_LAG)
        for t in range(t_tiles - RS_LAG, t_tiles):
            relay(t)
        if layer + 1 < num_layers:
            for p in range(n_q):
                q_copy(layer + 1, p).start()
        else:
            head_copy(1).start()

        last = layer + 1 == num_layers
        x_copies = []
        for t in range(t_tiles):
            for copy in rs_direct[t] + rs_final[t]:
                copy.wait_recv()
            cols = half_cols(core, t, TILE)
            for half in range(2):
                total = (y_sum[t, rows_of(chip, half), :] + direct_in[2 + half, t]) + direct_in[1 - half, t]
                x_new = (xg[rows_of(chip, half), cols].astype(F32) + total).astype(BF16)
                if last:
                    xg[rows_of(chip, half), cols] = x_new
                else:
                    x_full[half * rows:(half + 1) * rows, cols] = x_new
            if last:
                gather_start(t)
                if t >= AG_LAG:
                    gather_near(t - AG_LAG)
            else:
                copy = remote(x_full.at[:, cols], x_full.at[:, cols], x_send.at[1 + t], x_recv.at[1 + t], partner)
                copy.start()
                x_copies.append(copy)
        for copy in y_copies:
            copy.wait_send()
        for group in rs_relay + rs_direct + rs_final:
            for copy in group:
                copy.wait_send()
        for copy in x_copies:
            copy.wait()

    gather_end(t_tiles - AG_LAG, norm_final[0:1, :], out)
    head_copy(0).wait()
    head_copy(1).wait()


def head_kernel(h_ref, ahead, w_hbm, out_hbm, ring, stage, w_sem, out_sem):
    slots, _, tile = ring.shape
    per_s, per_a = slots // 2, 2
    per = per_s + per_a
    n_ahead = ahead.shape[1] // tile
    n_stream = w_hbm.shape[1] // tile - n_ahead
    n_steps = n_stream // per_s
    n_before, n_after = n_ahead - per_a * n_steps, n_stream - per_s * n_steps

    def col(t, c=0, n=tile):
        return pl.ds(pl.multiple_of(t * tile + c, TILE), n)

    def fetch(i, slot):
        return pltpu.make_async_copy(w_hbm.at[:, col(n_ahead + i)], ring.at[slot], w_sem.at[slot])

    def put(t, slot):
        return pltpu.make_async_copy(stage.at[slot], out_hbm.at[:, col(t)], out_sem.at[slot])

    def tiles(jobs):
        for t, weights, slot in jobs:
            for c in range(0, tile, TILE):
                stage[slot, :, c:c + TILE] = jnp.dot(h_ref[...], weights(c), preferred_element_type=F32)
        for t, weights, slot in jobs:
            put(t, slot).start()

    def from_ahead(i, slot):
        return i, lambda c: ahead[:, col(i, c, TILE)], slot

    def from_ring(i, ring_slot, slot):
        return n_ahead + i, lambda c: ring[ring_slot, :, c:c + TILE], slot

    for e in range(per_s):
        fetch(e, e).start()
    tiles([from_ahead(e, 2 * per + e) for e in range(n_before)])
    for e in range(per_s, slots):
        fetch(e, e).start()

    def step(i, carry):
        side = lax.rem(i, 2)
        for e in range(per_s):
            fetch(i * per_s + e, side * per_s + e).wait()

        @pl.when(i >= 2)
        def _():
            for e in range(per):
                put(0, side * per + e).wait()
        tiles([from_ring(i * per_s + e, side * per_s + e, side * per + e) for e in range(per_s)])
        for e in range(per_s):
            @pl.when(i * per_s + e + slots < n_stream)
            def _():
                fetch(i * per_s + e + slots, side * per_s + e).start()
        tiles([from_ahead(n_before + i * per_a + e, side * per + per_s + e) for e in range(per_a)])
        return carry

    lax.fori_loop(0, n_steps, step, 0)
    last = n_steps * per_s
    for e in range(n_after):
        fetch(last + e, (last + e) % slots).wait()
    for e in range(n_before):
        put(0, 2 * per + e).wait()
    tiles([from_ring(last + e, (last + e) % slots, 2 * per + e) for e in range(n_after)])
    for slot in range(2 * per + n_after):
        put(0, slot).wait()


def head_matmul(gathered, ahead, w_head):
    tile, slots, n_stage = 512, 6, 13
    depth, cols = w_head.shape
    rows = gathered.shape[0]
    hbm, vmem = pl.BlockSpec(memory_space=pl.ANY), pl.BlockSpec(memory_space=pltpu.VMEM)
    return pl.pallas_call(
        head_kernel,
        out_shape=jax.ShapeDtypeStruct((rows, cols), F32),
        in_specs=[vmem, vmem, hbm],
        out_specs=hbm,
        scratch_shapes=[pltpu.VMEM((slots, depth, tile), BF16), pltpu.VMEM((n_stage, rows, tile), F32),
                        pltpu.SemaphoreType.DMA((slots,)), pltpu.SemaphoreType.DMA((n_stage,))],
        compiler_params=pltpu.CompilerParams(vmem_limit_bytes=22 * 1024 * 1024),
        cost_estimate=pl.CostEstimate(flops=2 * rows * depth * cols, bytes_accessed=2 * depth * cols + 4 * rows * cols,
                                      transcendentals=0),
        name="head_matmul",
    )(gathered, ahead, w_head)


def decode_layers(n_dev, lengths, hidden, kv_cache, norm_attn, w_q, w_o, norm_ffn, w_gate, w_up, w_down, norm_final, w_head):
    num_layers, rows, seq_len, width = kv_cache.shape
    d_model = hidden.shape[1]
    heads = w_q.shape[2] // width
    ffn = w_gate.shape[2]
    pair, group_rows, half_d = 2 * rows, n_dev * rows, d_model // 2
    q_cols = heads * width // 2
    wa_cols = max(q_cols, 2 * ffn + d_model)
    wa_cols = -(-wa_cols // LANES) * LANES
    t_tiles = half_d // TILE
    pad_width = -(-width // LANES) * LANES
    hbm, vmem = pl.BlockSpec(memory_space=pl.ANY), pl.BlockSpec(memory_space=pltpu.VMEM)
    smem = pl.BlockSpec(memory_space=pltpu.SMEM)
    dma = pltpu.SemaphoreType.DMA
    cfg = (num_layers, rows, heads, width, d_model, ffn, n_dev)
    n_q = q_cols // (2 * width)
    scratch = [
        pltpu.VMEM((rows, width, seq_len), BF16),
        pltpu.VMEM((pair, d_model), BF16),
        pltpu.VMEM((pair, d_model), BF16),
        pltpu.VMEM((pad_width // LANES, heads * pair, LANES), F32),
        pltpu.VMEM((LATENT_DIM // LANES, heads * rows, LANES), F32),
        pltpu.VMEM((pair, heads * LATENT_DIM), BF16),
        pltpu.VMEM((group_rows, d_model), BF16),
        pltpu.VMEM((group_rows, ffn), BF16),
        pltpu.VMEM((t_tiles, group_rows, TILE), F32),
        pltpu.VMEM((t_tiles, group_rows, TILE), F32),
        pltpu.VMEM((t_tiles, group_rows, TILE), F32),
        pltpu.VMEM((2, t_tiles, rows, TILE), F32),
        pltpu.VMEM((2, t_tiles, rows, TILE), F32),
        pltpu.VMEM((4, t_tiles, rows, TILE), F32),
        dma((n_q + 4 + 3,)),
        dma((rows // GROUP,)),
        dma((2,)),
        dma((1 + t_tiles,)), dma((1 + t_tiles,)),
        dma((2 * n_q,)), dma((2 * n_q,)),
        dma((2,)), dma((2,)),
        dma((6, t_tiles)), dma((6, t_tiles)),
        dma((7, t_tiles)), dma((7, t_tiles)),
        dma((t_tiles,)), dma((t_tiles,)),
        dma((6, t_tiles)), dma((6, t_tiles)),
    ]
    gathered, ahead = pl.pallas_call(
        functools.partial(decode_kernel, cfg),
        out_shape=(pltpu.VMEM((group_rows, d_model), BF16), pltpu.VMEM((d_model, wa_cols + w_o.shape[1] // d_model * half_d), BF16)),
        in_specs=[smem, vmem, hbm, vmem, hbm, hbm, vmem, hbm, hbm, hbm, vmem, hbm],
        out_specs=(vmem, vmem),
        scratch_shapes=scratch,
        compiler_params=pltpu.CompilerParams(collective_id=0, has_side_effects=True, vmem_limit_bytes=26 * 1024 * 1024),
        name="decode_layers",
    )(lengths, hidden, jnp.swapaxes(kv_cache, 2, 3), norm_attn, w_q, w_o, norm_ffn, w_gate, w_up, w_down, norm_final.reshape(1, -1), w_head)
    gathered, ahead = (pltpu.with_memory_space_constraint(a, pltpu.VMEM) for a in (gathered, ahead))
    return head_matmul(gathered, ahead, w_head)


def solution(mesh):
    row_axes = ('rep', 'dp')
    specs_in = (P(row_axes, None), P(row_axes), P(None, row_axes, None, None), P(), P(), P(), P(),
                P(None, None, 'dp'), P(None, None, 'dp'), P(None, 'dp', None), P(), P(None, 'dp'))
    n_dev = mesh.shape['dp']

    def device_step(hidden, lengths, kv_cache, norm_attn, w_q, w_o, norm_ffn, w_gate, w_up, w_down, norm_final, w_head):
        return decode_layers(n_dev, lengths, hidden, kv_cache, norm_attn, w_q, w_o, norm_ffn, w_gate, w_up, w_down,
                             norm_final, w_head)

    return jax.shard_map(device_step, mesh=mesh, in_specs=specs_in, out_specs=P('rep', 'dp'), check_vma=False)
```
